32 devices in a mesh: gz: 4 (over x, core), xy: 8 (over z, y).
Axes of the slice: x: 2, y: 2, z: 4, core: 2. Of those that a mesh axis runs over, the one named last changes fastest.
Arguments:
- thermal_load: float32 [64, 4, 128, 384], P('gz', None, 'xy'), may hold values from -12 to 12
- material: int32 [64, 128, 384], P('gz', 'xy'), may hold values from 0 to 7
- layer_ids: int32 [64, 128, 384], P('gz', 'xy'), may hold values from 0 to 5
- stiffness: float32 [8, 4, 4], replicated, may hold values from -0.7 to 13, as said below
- coupling: float32 [6, 4, 4], replicated, may hold values from -0.15 to 0.9, as said below
- pivots: float32 [8, 4, 4], replicated, may hold values from -0.015 to 0.14, as said below
- factor: float32 [6, 4, 4], replicated, may hold values from -0.01 to 1
Outputs:
- solution: float32 [64, 4, 128, 384], P('gz', None, 'xy')
- residual: float32 [64, 4, 128, 384], P('gz', None, 'xy')
The draws below stay inside these ranges and needn't reach their ends.
Inputs may be any that keep to these rules, and one draw needn't show every extreme that they name: `stiffness`: each block is symmetric, and the operator A of the steps is positive definite. `coupling`: each block is symmetric. `pivots`: each block is symmetric positive definite.
All inputs are finite; a program needn't handle non-finite values.
Results may differ from the reference program's by a relative error of at most 0.0003.
Values sent between devices are 32-bit elements; how exact they have to be, the bound alone decides.
A program may use at most 192 MiB of HBM per device.

```python
import jax
import jax.numpy as jnp
from jax import lax

NY = 384
NMAT = 8
NLAY = 6
ITERS = 2
THICKNESS_CELLS = 64
NX = 128


def symmetric_offdiag(subkey, table_entries, spread):
    sampled = jax.random.uniform(subkey, (table_entries, 4, 4), jnp.float32, -spread, spread)
    upper_part = jnp.triu(sampled, 1)
    return upper_part + jnp.swapaxes(upper_part, 1, 2)


def with_diagonal(offdiag, diagonal_values):
    return offdiag + diagonal_values[:, :, None] * jnp.eye(4, dtype=jnp.float32)[None]


def draw_thermal_load(key, part):
    random_subkey_list = jax.random.split(key, 1)
    depth_frac = jnp.arange(THICKNESS_CELLS, dtype=jnp.float32) / max(THICKNESS_CELLS - 1, 1)
    width_frac = jnp.arange(NX, dtype=jnp.float32) / max(NX - 1, 1)
    scaling = jnp.exp(0.5 * jnp.log(3.0) * (depth_frac[:, None, None, None] + width_frac[None, None, :, None]))
    sampled = jax.random.normal(random_subkey_list[0], (THICKNESS_CELLS, 4, NX, NY), jnp.float32)
    return jnp.clip(sampled * scaling, -12.0, 12.0)


def draw_layer_ids(key, part):
    random_subkey_list = jax.random.split(key, 4)
    planes = jax.random.randint(random_subkey_list[0], (THICKNESS_CELLS,), 0, NLAY - 1)
    scattered = jax.random.randint(random_subkey_list[1], (THICKNESS_CELLS, NX, NY), 0, NLAY - 1)
    picked = jax.random.randint(random_subkey_list[2], (THICKNESS_CELLS, NX, NY), 0, 4) == 0
    labels = jnp.where(picked, scattered, planes[:, None, None])
    split_groups = jax.random.randint(random_subkey_list[3], (2,), 0, THICKNESS_CELLS)
    depth_levels = jnp.arange(THICKNESS_CELLS, dtype=jnp.int32)
    splitting_apart = jnp.any(depth_levels[:, None] == split_groups[None, :], axis=1)
    return jnp.where(splitting_apart[:, None, None], NLAY - 1, labels).astype(jnp.int32)


def draw_stiffness(key, part):
    random_subkey_list = jax.random.split(key, 2)
    diagonal_values = jax.random.uniform(random_subkey_list[1], (NMAT, 4), jnp.float32, 9.0, 13.0)
    return with_diagonal(symmetric_offdiag(random_subkey_list[0], NMAT, 0.7), diagonal_values)


def draw_coupling(key, part):
    random_subkey_list = jax.random.split(key, 2)
    diagonal_values = jax.random.uniform(random_subkey_list[1], (NLAY, 4), jnp.float32, 0.3, 0.9)
    return with_diagonal(symmetric_offdiag(random_subkey_list[0], NLAY, 0.15), diagonal_values)


def draw_pivots(key, part):
    random_subkey_list = jax.random.split(key, 2)
    diagonal_values = jax.random.uniform(random_subkey_list[1], (NMAT, 4), jnp.float32, 0.06, 0.14)
    return with_diagonal(symmetric_offdiag(random_subkey_list[0], NMAT, 0.015), diagonal_values)


def draw_factor(key, part):
    random_subkey_list = jax.random.split(key, 6)
    ordering = jax.random.permutation(random_subkey_list[0], 4)
    keeping = 2
    slow_flag = jnp.zeros((4,), jnp.float32).at[ordering[:keeping]].set(1.0)
    slow_rate = jax.random.uniform(random_subkey_list[1], (4,), jnp.float32, 0.05, 0.3) / THICKNESS_CELLS
    fast_rate = 1.0 / jax.random.uniform(random_subkey_list[2], (4,), jnp.float32, 30.0, 50.0)
    base_rate = jnp.where(slow_flag > 0.5, slow_rate, fast_rate)
    stretch = jax.random.uniform(random_subkey_list[3], (NLAY, 4), jnp.float32, 0.5, 2.0)
    diagonal_values = jnp.exp(-base_rate[None, :] * stretch)
    splitting_apart = jax.random.uniform(random_subkey_list[4], (4,), jnp.float32, 0.6, 0.85)
    diagonal_values = diagonal_values.at[NLAY - 1].multiply(splitting_apart)
    offdiag = jax.random.uniform(random_subkey_list[5], (NLAY, 4, 4), jnp.float32, -0.25, 0.25) / THICKNESS_CELLS
    offdiag = offdiag * (1.0 - jnp.eye(4, dtype=jnp.float32))[None]
    return with_diagonal(offdiag, diagonal_values)


def place_ends(drawn, own_key, least, largest):
    index_at = [jax.random.randint(jax.random.fold_in(own_key, axis), (), 0, length) for axis, length in enumerate(drawn.shape)]
    widest = drawn.shape.index(max(drawn.shape))
    beside = index_at[:widest] + [(index_at[widest] + 1) % drawn.shape[widest]] + index_at[widest + 1:]
    return drawn.at[tuple(index_at)].set(least).at[tuple(beside)].set(largest)


def setup_inputs(seed: int = 0) -> dict:
    seeds = jax.random.split(jax.random.key(seed), 8)
    thermal_load = draw_thermal_load(jax.random.fold_in(seeds[7], 71), 0)
    material = place_ends(jax.random.randint(seeds[1], (THICKNESS_CELLS, NX, NY), 0, NMAT), jax.random.fold_in(seeds[1], 1), 0, NMAT - 1).astype(jnp.int32)
    layer_ids = draw_layer_ids(jax.random.fold_in(seeds[7], 71), 0)
    stiffness = draw_stiffness(jax.random.fold_in(seeds[7], 71), 0)
    coupling = draw_coupling(jax.random.fold_in(seeds[7], 71), 0)
    pivots = draw_pivots(jax.random.fold_in(seeds[7], 71), 0)
    factor = draw_factor(jax.random.fold_in(seeds[7], 71), 0)
    return dict(thermal_load=thermal_load, material=material, layer_ids=layer_ids, stiffness=stiffness, coupling=coupling, pivots=pivots, factor=factor)


def apply_table(blocks_table, labels, vectors):
    summed = jnp.zeros_like(vectors)
    for table_row in range(blocks_table.shape[0]):
        product_rows = jnp.einsum("ij,...jxy->...ixy", blocks_table[table_row], vectors, precision=lax.Precision.HIGHEST)
        chosen = jnp.expand_dims(labels == table_row, -3)
        summed = summed + jnp.where(chosen, product_rows, jnp.zeros_like(product_rows))
    return summed


def operate(field, material, layer_ids, stiffness, coupling):
    result_rows = apply_table(stiffness, material, field)
    pushed = apply_table(coupling, layer_ids, field)
    plane_zero = jnp.zeros_like(field[:1])
    upper_field = jnp.concatenate([field[1:], plane_zero], axis=0)
    lower_pushed = jnp.concatenate([plane_zero, pushed[:-1]], axis=0)
    padded = jnp.pad(field, ((0, 0), (0, 0), (1, 1), (1, 1)))
    beside = padded[:, :, 2:, 1:-1] + padded[:, :, :-2, 1:-1]
    beside = beside + padded[:, :, 1:-1, 2:] + padded[:, :, 1:-1, :-2]
    from_upper = apply_table(coupling, layer_ids, upper_field)
    return result_rows - beside - from_upper - lower_pushed


def precondition(residual, material, layer_ids, pivots, factor):
    zeros_plane = jnp.zeros(residual.shape[1:], jnp.float32)

    def forward(carried, paired):
        plane_rows, labels = paired
        updated = plane_rows + apply_table(factor, labels, carried)
        return updated, updated

    _, climbed = lax.scan(forward, zeros_plane, (residual, layer_ids))
    scaled = apply_table(pivots, material, climbed)
    transposed = jnp.swapaxes(factor, 1, 2)

    def backward(carried, paired):
        plane_rows, labels = paired
        updated = plane_rows + carried
        return apply_table(transposed, labels, updated), updated

    _, result_rows = lax.scan(backward, zeros_plane, (scaled, layer_ids), reverse=True)
    return result_rows


def reference(thermal_load, material, layer_ids, stiffness, coupling, pivots, factor):
    solution = jnp.zeros_like(thermal_load)
    residual = thermal_load
    precond = precondition(residual, material, layer_ids, pivots, factor)
    direction = precond
    precond_dot = jnp.sum(residual * precond)
    for iteration in range(ITERS):
        applied = operate(direction, material, layer_ids, stiffness, coupling)
        step_size = precond_dot / jnp.sum(direction * applied)
        solution = solution + step_size * direction
        residual = residual - step_size * applied
        if iteration + 1 < ITERS:
            precond = precondition(residual, material, layer_ids, pivots, factor)
            following_product = jnp.sum(residual * precond)
            direction = precond + (following_product / precond_dot) * direction
            precond_dot = following_product
    return solution, residual
```

```python
import functools

import jax
import jax.numpy as jnp
from jax import lax
from jax.experimental import pallas as pl
from jax.experimental.pallas import tpu as pltpu
from jax.sharding import PartitionSpec as P

MESH = pl.DeviceIdType.MESH
PAIRS = [(i, j) for i in range(4) for j in range(i, 4)]
SYM = {}
for _k, (_i, _j) in enumerate(PAIRS):
    SYM[_i, _j] = _k
    SYM[_j, _i] = _k
UP, DOWN, PUSH, PLANE, LOW, HIGH = range(6)


def pick(values, bits):
    level = 0
    while len(values) > 1:
        merged = []
        for i in range(0, len(values) - 1, 2):
            merged.append(jnp.where(bits[level], values[i + 1], values[i]))
        if len(values) % 2:
            merged.append(values[-1])
        values = merged
        level += 1
    return values[0]


def bit_masks(labels, entries):
    count = max(1, (entries - 1).bit_length())
    return [(labels & (1 << b)) != 0 for b in range(count)]


def total(terms):
    return (terms[0] + terms[1]) + (terms[2] + terms[3])


def kernel(
    n, m,
    load_ref, mat_ref, lay_ref, stiff_ref, coup_ref, piv_ref, fact_ref,
    sol_ref, res_ref,
    kc, cc, sc, pc, tc, u, au,
    up_send, up_recv, dn_send, dn_recv, push_send, push_recv, plane_recv,
    halo_send, halo_recv, gbuf, xbuf,
    send_sem, recv_sem, gs_sem, gr_sem, xs_sem, xr_sem,
):
    depth, _, nx, ny = load_ref.shape
    me = lax.axis_index("gz")
    side = lax.axis_index("xy")
    not_first, not_last = me > 0, me < n - 1
    has_left, has_right = side > 0, side < m - 1

    barrier = pltpu.get_barrier_semaphore()
    for k in range(1, n):
        pl.semaphore_signal(
            barrier, inc=1, device_id={"gz": lax.rem(me + k, n)}, device_id_type=MESH
        )
    for k in range(1, m):
        pl.semaphore_signal(
            barrier, inc=1, device_id={"xy": lax.rem(side + k, m)}, device_id_type=MESH
        )

    def neighbour(axis, step):
        if axis == "gz":
            return {"gz": lax.rem(me + step + n, n)}
        return {"xy": lax.rem(side + step + m, m)}

    def remote(src, dst, it, kind, axis, step):
        return pltpu.make_async_remote_copy(
            src_ref=src, dst_ref=dst, send_sem=send_sem.at[it, kind],
            recv_sem=recv_sem.at[it, kind], device_id=neighbour(axis, step),
            device_id_type=MESH,
        )

    def copy(it, kind):
        if kind == UP:
            return remote(up_send.at[it], up_recv.at[it], it, UP, "gz", 1)
        if kind == DOWN:
            return remote(dn_send.at[it], dn_recv.at[it], it, DOWN, "gz", -1)
        if kind == PUSH:
            return remote(push_send.at[it], push_recv.at[it], it, PUSH, "gz", 1)
        if kind == PLANE:
            return remote(u.at[it, 1], plane_recv.at[it], it, PLANE, "gz", -1)
        if kind == LOW:
            return remote(halo_send.at[it, 0], halo_recv.at[it, 1], it, LOW, "xy", -1)
        return remote(halo_send.at[it, 1], halo_recv.at[it, 0], it, HIGH, "xy", 1)

    senders = {UP: not_last, DOWN: not_first, PUSH: not_last, PLANE: not_first,
               LOW: has_left, HIGH: has_right}
    receivers = {UP: not_first, DOWN: not_last, PUSH: not_first, PLANE: not_last,
                 LOW: has_right, HIGH: has_left}

    def start(it, kind):
        @pl.when(senders[kind])
        def _():
            copy(it, kind).start()

    def arrive(it, kind):
        @pl.when(receivers[kind])
        def _():
            copy(it, kind).wait_recv()

    zero_plane = jnp.zeros((4, nx, ny), jnp.float32)

    @pl.when(me == 0)
    def _():
        for it in range(2):
            up_recv[it] = zero_plane
            push_recv[it] = zero_plane

    @pl.when(me == n - 1)
    def _():
        for it in range(2):
            dn_recv[it] = zero_plane
            plane_recv[it] = zero_plane

    @pl.when(side == 0)
    def _():
        for it in range(2):
            halo_recv[it, 0] = jnp.zeros((depth, 4, ny), jnp.float32)

    @pl.when(side == m - 1)
    def _():
        for it in range(2):
            halo_recv[it, 1] = jnp.zeros((depth, 4, ny), jnp.float32)

    for it in range(2):
        u[it, 0] = zero_plane
        u[it, depth + 1] = zero_plane
    for k in range(10):
        cc[0, k] = jnp.zeros((nx, ny), jnp.float32)

    def fill(table, label_ref, out, entries_of, offset):
        entries = table.shape[0]

        def plane(z, carry):
            for t in range(0, ny, 128):
                bits = bit_masks(label_ref[z, :, t:t + 128], entries)
                for k, (i, j) in enumerate(entries_of):
                    values = [
                        jnp.full((nx, 128), table[e, i, j], jnp.float32) for e in range(entries)
                    ]
                    out[z + offset, k, :, t:t + 128] = pick(values, bits)
            return carry

        lax.fori_loop(0, depth, plane, 0)

    def fill_rest():
        fill(piv_ref, mat_ref, sc, PAIRS, 0)
        fill(stiff_ref, mat_ref, kc, PAIRS, 0)
        fill(coup_ref, lay_ref, cc, PAIRS, 1)

    fill(fact_ref, lay_ref, pc, [(i, j) for i in range(4) for j in range(4)], 0)

    def sym_apply(ref, z, v):
        return [total([ref[z, SYM[i, j]] * v[j] for j in range(4)]) for i in range(4)]

    def lift(z, v):
        return [total([pc[z, 4 * i + j] * v[j] for j in range(4)]) for i in range(4)]

    def drop(z, v):
        return [total([pc[z, 4 * j + i] * v[j] for j in range(4)]) for i in range(4)]

    def zeros4():
        return tuple(jnp.zeros((nx, ny), jnp.float32) for _ in range(4))

    def climb(src, it, z, carried, keep):
        moved = lift(z, carried)
        carried = [src[z, c] + moved[c] for c in range(4)]
        if keep:
            scaled = sym_apply(sc, z, carried)
            for c in range(4):
                u[it, z + 1, c] = scaled[c]
        return tuple(carried)

    def build_transfer():
        for x in range(0, nx, 8):
            for t in range(0, ny, 128):
                def level(z, now):
                    p = [pc[z, k, x:x + 8, t:t + 128] for k in range(16)]
                    return tuple(
                        total([p[4 * i + k] * now[4 * k + j] for k in range(4)])
                        for i in range(4) for j in range(4)
                    )

                now = tuple(pc[0, k, x:x + 8, t:t + 128] for k in range(16))
                now = lax.fori_loop(1, depth, level, now)
                for k in range(16):
                    tc[k, x:x + 8, t:t + 128] = now[k]

    def precondition(src, it):
        out = lax.fori_loop(
            0, depth, lambda z, c: climb(src, it, z, c, False), zeros4()
        )
        for c in range(4):
            up_send[it, c] = out[c]
        if it == 0:
            pl.semaphore_wait(barrier, n - 1 + m - 1)

        @pl.when(me == 0)
        def _():
            copy(it, UP).start()

        if it == 0:
            build_transfer()

            @pl.when(me >= n // 2)
            def _():
                fill_rest()

        @pl.when(not_first)
        def _():
            copy(it, UP).wait_recv()

            @pl.when(not_last)
            def _():
                for i in range(4):
                    moved = total([tc[4 * i + j] * up_recv[it, j] for j in range(4)])
                    up_send[it, i] = up_send[it, i] + moved
                copy(it, UP).start()

        if it == 0:
            @pl.when(me < n // 2)
            def _():
                fill_rest()

        inflow = tuple(up_recv[it, c] for c in range(4))
        lax.fori_loop(0, depth, lambda z, c: climb(src, it, z, c, True), inflow)

        def fall(k, carried):
            z = depth - 1 - k
            return tuple(drop(z, [u[it, z + 1, c] + carried[c] for c in range(4)]))

        out = lax.fori_loop(0, depth, fall, zeros4())
        for c in range(4):
            dn_send[it, c] = out[c]

        @pl.when(me == n - 1)
        def _():
            copy(it, DOWN).start()

        @pl.when(not_last)
        def _():
            copy(it, DOWN).wait_recv()

            @pl.when(not_first)
            def _():
                for i in range(4):
                    moved = total([tc[4 * j + i] * dn_recv[it, j] for j in range(4)])
                    dn_send[it, i] = dn_send[it, i] + moved
                copy(it, DOWN).start()

        def settle(k, carried):
            z = depth - 1 - k
            now = [u[it, z + 1, c] + carried[c] for c in range(4)]
            for c in range(4):
                u[it, z + 1, c] = now[c]
            halo_send[it, 0, z] = jnp.concatenate([v[0:1] for v in now], axis=0)
            halo_send[it, 1, z] = jnp.concatenate([v[nx - 1:nx] for v in now], axis=0)
            return tuple(drop(z, now))

        inflow = tuple(dn_recv[it, c] for c in range(4))
        lax.fori_loop(0, depth, settle, inflow)
        start(it, LOW)
        start(it, HIGH)
        start(it, PLANE)
        pushed = sym_apply(cc, depth, [u[it, depth, c] for c in range(4)])
        for c in range(4):
            push_send[it, c] = pushed[c]
        start(it, PUSH)

    def operate(src, it):
        rows = lax.broadcasted_iota(jnp.int32, (nx, ny), 0)
        lanes = lax.broadcasted_iota(jnp.int32, (nx, ny), 1)

        def plane(z, carry):
            own, curve = carry
            here = [u[it, z + 1, c] for c in range(4)]
            above = [u[it, z + 2, c] for c in range(4)]
            below = [u[it, z, c] for c in range(4)]
            for c in range(4):
                v = here[c]
                acc = total([kc[z, SYM[c, j]] * here[j] for j in range(4)])
                acc = acc - total([cc[z + 1, SYM[c, j]] * above[j] for j in range(4)])
                acc = acc - total([cc[z, SYM[c, j]] * below[j] for j in range(4)])
                acc = acc - jnp.where(rows == 0, 0.0, pltpu.roll(v, 1, 0))
                acc = acc - jnp.where(rows == nx - 1, 0.0, pltpu.roll(v, nx - 1, 0))
                acc = acc - jnp.where(lanes == 0, 0.0, pltpu.roll(v, 1, 1))
                acc = acc - jnp.where(lanes == ny - 1, 0.0, pltpu.roll(v, ny - 1, 1))
                au[it, z, c] = acc
                own = own + src[z, c] * v
                curve = curve + v * acc
            return own, curve

        zero = jnp.zeros((nx, ny), jnp.float32)
        own, curve = lax.fori_loop(0, depth, plane, (zero, zero))
        for kind in (PLANE, PUSH, LOW, HIGH):
            arrive(it, kind)
        upper = sym_apply(cc, depth, [plane_recv[it, c] for c in range(4)])
        for c in range(4):
            au[it, depth - 1, c] = au[it, depth - 1, c] - upper[c]
            curve = curve - u[it, depth, c] * upper[c]
            lower = push_recv[it, c]
            au[it, 0, c] = au[it, 0, c] - lower
            curve = curve - u[it, 1, c] * lower

        def edges(z, sums):
            for c in range(4):
                low = halo_recv[it, 0, z, c:c + 1]
                high = halo_recv[it, 1, z, c:c + 1]
                au[it, z, c, 0:1] = au[it, z, c, 0:1] - low
                au[it, z, c, nx - 1:nx] = au[it, z, c, nx - 1:nx] - high
                sums = sums + u[it, z + 1, c, 0:1] * low + u[it, z + 1, c, nx - 1:nx] * high
            return sums

        crossing = lax.fori_loop(0, depth, edges, jnp.zeros((1, ny), jnp.float32))

        def narrow(row):
            folded = row[:, 0:128]
            for t in range(128, ny, 128):
                folded = folded + row[:, t:t + 128]
            return folded

        own = narrow(jnp.sum(own, axis=0, keepdims=True))
        curve = narrow(jnp.sum(curve, axis=0, keepdims=True) - crossing)
        row = lax.broadcasted_iota(jnp.int32, (8, 128), 0)
        tile = jnp.where(row < 4, jnp.broadcast_to(own, (8, 128)), jnp.broadcast_to(curve, (8, 128)))
        for buf, ss, rs, axis, count, mine in (
            (gbuf, gs_sem, gr_sem, "gz", n, me), (xbuf, xs_sem, xr_sem, "xy", m, side)
        ):
            buf[it, mine] = tile
            for k in range(1, count):
                gather(buf, ss, rs, axis, mine, it, k).start()
            for k in range(1, count):
                gather(buf, ss, rs, axis, mine, it, k).wait_recv()
            tile = buf[it, 0]
            for k in range(1, count):
                tile = tile + buf[it, k]
        return (jnp.full((nx, ny), jnp.sum(tile[0:1]), jnp.float32),
                jnp.full((nx, ny), jnp.sum(tile[4:5]), jnp.float32))

    def gather(buf, ss, rs, axis, mine, it, k):
        return pltpu.make_async_remote_copy(
            src_ref=buf.at[it, mine], dst_ref=buf.at[it, mine], send_sem=ss.at[it, k],
            recv_sem=rs.at[it, k], device_id=neighbour(axis, k), device_id_type=MESH,
        )

    precondition(load_ref, 0)
    gamma, curve = operate(load_ref, 0)
    alpha = gamma / curve

    def update(z, carry):
        for c in range(4):
            res_ref[z, c] = load_ref[z, c] - alpha * au[0, z, c]
        return carry

    lax.fori_loop(0, depth, update, 0)
    precondition(res_ref, 1)
    fresh, curve = operate(res_ref, 1)
    beta = fresh / gamma
    second = fresh / (curve - beta * fresh / alpha)
    first = alpha + second * beta
    both = second * beta

    def finish(z, carry):
        for c in range(4):
            sol_ref[z, c] = first * u[0, z + 1, c] + second * u[1, z + 1, c]
            res_ref[z, c] = res_ref[z, c] - (second * au[1, z, c] + both * au[0, z, c])
        return carry

    lax.fori_loop(0, depth, finish, 0)
    for it in range(2):
        for kind in range(6):
            @pl.when(senders[kind])
            def _(it=it, kind=kind):
                copy(it, kind).wait_send()
        for buf, ss, rs, axis, count, mine in (
            (gbuf, gs_sem, gr_sem, "gz", n, me), (xbuf, xs_sem, xr_sem, "xy", m, side)
        ):
            for k in range(1, count):
                gather(buf, ss, rs, axis, mine, it, k).wait_send()


def solution(mesh):
    n, m = mesh.shape["gz"], mesh.shape["xy"]

    def per_device(load, material, layers, stiffness, coupling, pivots, factor):
        depth, _, nx, ny = load.shape
        f32 = jnp.float32
        vmem = pl.BlockSpec(memory_space=pltpu.VMEM)
        smem = pl.BlockSpec(memory_space=pltpu.SMEM)
        dma = pltpu.SemaphoreType.DMA
        edge = pltpu.VMEM((2, 4, nx, ny), f32)
        return pl.pallas_call(
            functools.partial(kernel, n, m),
            out_shape=(jax.ShapeDtypeStruct(load.shape, f32),) * 2,
            in_specs=[vmem] * 3 + [smem] * 4,
            out_specs=(vmem, vmem),
            scratch_shapes=[
                pltpu.VMEM((depth, 10, nx, ny), f32),
                pltpu.VMEM((depth + 1, 10, nx, ny), f32),
                pltpu.VMEM((depth, 10, nx, ny), f32),
                pltpu.VMEM((depth, 16, nx, ny), f32),
                pltpu.VMEM((16, nx, ny), f32),
                pltpu.VMEM((2, depth + 2, 4, nx, ny), f32),
                pltpu.VMEM((2, depth, 4, nx, ny), f32),
                edge, edge, edge, edge, edge, edge, edge,
                pltpu.VMEM((2, 2, depth, 4, ny), f32),
                pltpu.VMEM((2, 2, depth, 4, ny), f32),
                pltpu.VMEM((2, n, 8, 128), f32),
                pltpu.VMEM((2, m, 8, 128), f32),
                dma((2, 6)), dma((2, 6)),
                dma((2, n)), dma((2, n)), dma((2, m)), dma((2, m)),
            ],
            compiler_params=pltpu.CompilerParams(
                collective_id=0, has_side_effects=True, vmem_limit_bytes=58 * 1024 * 1024
            ),
            name="line_cg",
        )(load, material, layers, stiffness, coupling, pivots, factor)

    split = P("gz", None, "xy", None)
    labels = P("gz", "xy", None)
    return jax.shard_map(
        per_device,
        mesh=mesh,
        in_specs=(split, labels, labels, P(), P(), P(), P()),
        out_specs=(split, split),
        check_vma=False,
    )
```

```python
import functools

import jax
import jax.numpy as jnp
from jax import lax
from jax.experimental import pallas as pl
from jax.experimental.pallas import tpu as pltpu
from jax.sharding import PartitionSpec as P

MESH = pl.DeviceIdType.MESH
PAIRS = [(i, j) for i in range(4) for j in range(i, 4)]
SYM = {}
for _k, (_i, _j) in enumerate(PAIRS):
    SYM[_i, _j] = _k
    SYM[_j, _i] = _k
UP, DOWN, PUSH, PLANE, LOW, HIGH = range(6)


def pick(values, bits):
    level = 0
    while len(values) > 1:
        merged = []
        for i in range(0, len(values) - 1, 2):
            merged.append(jnp.where(bits[level], values[i + 1], values[i]))
        if len(values) % 2:
            merged.append(values[-1])
        values = merged
        level += 1
    return values[0]


def bit_masks(labels, entries):
    count = max(1, (entries - 1).bit_length())
    return [(labels & (1 << b)) != 0 for b in range(count)]


def total(terms):
    return (terms[0] + terms[1]) + (terms[2] + terms[3])


def kernel(
    n, m,
    load_ref, mat_ref, lay_ref, stiff_ref, coup_ref, piv_ref, fact_ref,
    base_ref, image_ref, turn_ref, bend_ref, scalar_ref,
    kc, cc, sc, pc, tc, u, au,
    up_send, up_recv, dn_send, dn_recv, push_send, push_recv, plane_recv,
    halo_send, halo_recv, gbuf, xbuf,
    send_sem, recv_sem, gs_sem, gr_sem, xs_sem, xr_sem, out_sem,
):
    depth, _, nx, ny = load_ref.shape
    me = lax.axis_index("gz")
    side = lax.axis_index("xy")
    not_first, not_last = me > 0, me < n - 1
    has_left, has_right = side > 0, side < m - 1

    barrier = pltpu.get_barrier_semaphore()
    for k in range(1, n):
        pl.semaphore_signal(
            barrier, inc=1, device_id={"gz": lax.rem(me + k, n)}, device_id_type=MESH
        )
    for k in range(1, m):
        pl.semaphore_signal(
            barrier, inc=1, device_id={"xy": lax.rem(side + k, m)}, device_id_type=MESH
        )

    def neighbour(axis, step):
        if axis == "gz":
            return {"gz": lax.rem(me + step + n, n)}
        return {"xy": lax.rem(side + step + m, m)}

    def remote(src, dst, it, kind, axis, step):
        return pltpu.make_async_remote_copy(
            src_ref=src, dst_ref=dst, send_sem=send_sem.at[it, kind],
            recv_sem=recv_sem.at[it, kind], device_id=neighbour(axis, step),
            device_id_type=MESH,
        )

    def copy(it, kind):
        if kind == UP:
            return remote(up_send.at[it], up_recv.at[it], it, UP, "gz", 1)
        if kind == DOWN:
            return remote(dn_send.at[it], dn_recv.at[it], it, DOWN, "gz", -1)
        if kind == PUSH:
            return remote(push_send.at[it], push_recv.at[it], it, PUSH, "gz", 1)
        if kind == PLANE:
            return remote(u.at[it, 1], plane_recv.at[it], it, PLANE, "gz", -1)
        if kind == LOW:
            return remote(halo_send.at[it, 0], halo_recv.at[it, 1], it, LOW, "xy", -1)
        return remote(halo_send.at[it, 1], halo_recv.at[it, 0], it, HIGH, "xy", 1)

    senders = {UP: not_last, DOWN: not_first, PUSH: not_last, PLANE: not_first,
               LOW: has_left, HIGH: has_right}
    receivers = {UP: not_first, DOWN: not_last, PUSH: not_first, PLANE: not_last,
                 LOW: has_right, HIGH: has_left}

    def start(it, kind):
        @pl.when(senders[kind])
        def _():
            copy(it, kind).start()

    def arrive(it, kind):
        @pl.when(receivers[kind])
        def _():
            copy(it, kind).wait_recv()

    zero_plane = jnp.zeros((4, nx, ny), jnp.float32)

    @pl.when(me == 0)
    def _():
        for it in range(2):
            up_recv[it] = zero_plane
            push_recv[it] = zero_plane

    @pl.when(me == n - 1)
    def _():
        for it in range(2):
            dn_recv[it] = zero_plane
            plane_recv[it] = zero_plane

    @pl.when(side == 0)
    def _():
        for it in range(2):
            halo_recv[it, 0] = jnp.zeros((depth, 4, ny), jnp.float32)

    @pl.when(side == m - 1)
    def _():
        for it in range(2):
            halo_recv[it, 1] = jnp.zeros((depth, 4, ny), jnp.float32)

    for it in range(2):
        u[it, 0] = zero_plane
        u[it, depth + 1] = zero_plane
    for k in range(10):
        cc[0, k] = jnp.zeros((nx, ny), jnp.float32)

    def fill(table, label_ref, out, entries_of, offset):
        entries = table.shape[2]

        def plane(z, carry):
            for t in range(0, ny, 128):
                bits = bit_masks(label_ref[z, :, t:t + 128], entries)
                for k, (i, j) in enumerate(entries_of):
                    values = [
                        jnp.full((nx, 128), table[i, j, e], jnp.float32) for e in range(entries)
                    ]
                    out[z + offset, k, :, t:t + 128] = pick(values, bits)
            return carry

        lax.fori_loop(0, depth, plane, 0)

    def fill_rest():
        fill(piv_ref, mat_ref, sc, PAIRS, 0)
        fill(stiff_ref, mat_ref, kc, PAIRS, 0)
        fill(coup_ref, lay_ref, cc, PAIRS, 1)

    fill(fact_ref, lay_ref, pc, [(i, j) for i in range(4) for j in range(4)], 0)

    def sym_apply(ref, z, v):
        return [total([ref[z, SYM[i, j]] * v[j] for j in range(4)]) for i in range(4)]

    def lift(z, v):
        return [total([pc[z, 4 * i + j] * v[j] for j in range(4)]) for i in range(4)]

    def drop(z, v):
        return [total([pc[z, 4 * j + i] * v[j] for j in range(4)]) for i in range(4)]

    def zeros4():
        return tuple(jnp.zeros((nx, ny), jnp.float32) for _ in range(4))

    def climb(src, it, z, carried, keep):
        moved = lift(z, carried)
        carried = [src[z, c] + moved[c] for c in range(4)]
        if keep:
            scaled = sym_apply(sc, z, carried)
            for c in range(4):
                u[it, z + 1, c] = scaled[c]
        return tuple(carried)

    def build_transfer():
        for x in range(0, nx, 8):
            for t in range(0, ny, 128):
                def level(z, now):
                    p = [pc[z, k, x:x + 8, t:t + 128] for k in range(16)]
                    return tuple(
                        total([p[4 * i + k] * now[4 * k + j] for k in range(4)])
                        for i in range(4) for j in range(4)
                    )

                now = tuple(pc[0, k, x:x + 8, t:t + 128] for k in range(16))
                now = lax.fori_loop(1, depth, level, now)
                for k in range(16):
                    tc[k, x:x + 8, t:t + 128] = now[k]

    def precondition(src, it):
        out = lax.fori_loop(
            0, depth, lambda z, c: climb(src, it, z, c, False), zeros4()
        )
        for c in range(4):
            up_send[it, c] = out[c]
        if it == 0:
            pl.semaphore_wait(barrier, n - 1 + m - 1)

        @pl.when(me == 0)
        def _():
            copy(it, UP).start()

        if it == 0:
            build_transfer()

            @pl.when(me >= n // 2)
            def _():
                fill_rest()

        @pl.when(not_first)
        def _():
            copy(it, UP).wait_recv()

            @pl.when(not_last)
            def _():
                for i in range(4):
                    moved = total([tc[4 * i + j] * up_recv[it, j] for j in range(4)])
                    up_send[it, i] = up_send[it, i] + moved
                copy(it, UP).start()

        if it == 0:
            @pl.when(me < n // 2)
            def _():
                fill_rest()

        else:
            reduce_across(it - 1)

        inflow = tuple(up_recv[it, c] for c in range(4))
        lax.fori_loop(0, depth, lambda z, c: climb(src, it, z, c, True), inflow)

        def fall(k, carried):
            z = depth - 1 - k
            return tuple(drop(z, [u[it, z + 1, c] + carried[c] for c in range(4)]))

        out = lax.fori_loop(0, depth, fall, zeros4())
        for c in range(4):
            dn_send[it, c] = out[c]

        @pl.when(me == n - 1)
        def _():
            copy(it, DOWN).start()

        @pl.when(not_last)
        def _():
            copy(it, DOWN).wait_recv()

            @pl.when(not_first)
            def _():
                for i in range(4):
                    moved = total([tc[4 * j + i] * dn_recv[it, j] for j in range(4)])
                    dn_send[it, i] = dn_send[it, i] + moved
                copy(it, DOWN).start()

        def settle(k, carried):
            z = depth - 1 - k
            now = [u[it, z + 1, c] + carried[c] for c in range(4)]
            for c in range(4):
                u[it, z + 1, c] = now[c]
            halo_send[it, 0, z] = jnp.concatenate([v[0:1] for v in now], axis=0)
            halo_send[it, 1, z] = jnp.concatenate([v[nx - 1:nx] for v in now], axis=0)
            return tuple(drop(z, now))

        inflow = tuple(dn_recv[it, c] for c in range(4))
        pushed = sym_apply(cc, depth, [u[it, depth, c] + inflow[c] for c in range(4)])
        for c in range(4):
            push_send[it, c] = pushed[c]
        start(it, PUSH)
        lax.fori_loop(0, depth, settle, inflow)
        start(it, LOW)
        start(it, HIGH)
        start(it, PLANE)
        deliver(it).start()

    def deliver(it):
        target = (base_ref, turn_ref)[it]
        return pltpu.make_async_copy(u.at[it, pl.ds(1, depth)], target, out_sem.at[it])

    def deliver_image(it):
        target = (image_ref, bend_ref)[it]
        return pltpu.make_async_copy(au.at[it], target, out_sem.at[2 + it])

    def operate(it, alpha):
        rows = lax.broadcasted_iota(jnp.int32, (nx, ny), 0)
        lanes = lax.broadcasted_iota(jnp.int32, (nx, ny), 1)

        def plane(z, carry):
            own, curve = carry
            here = [u[it, z + 1, c] for c in range(4)]
            above = [u[it, z + 2, c] for c in range(4)]
            below = [u[it, z, c] for c in range(4)]
            for c in range(4):
                v = here[c]
                acc = total([kc[z, SYM[c, j]] * here[j] for j in range(4)])
                acc = acc - total([cc[z + 1, SYM[c, j]] * above[j] for j in range(4)])
                acc = acc - total([cc[z, SYM[c, j]] * below[j] for j in range(4)])
                acc = acc - jnp.where(rows == 0, 0.0, pltpu.roll(v, 1, 0))
                acc = acc - jnp.where(rows == nx - 1, 0.0, pltpu.roll(v, nx - 1, 0))
                acc = acc - jnp.where(lanes == 0, 0.0, pltpu.roll(v, 1, 1))
                acc = acc - jnp.where(lanes == ny - 1, 0.0, pltpu.roll(v, ny - 1, 1))
                au[it, z, c] = acc
                if it == 0:
                    own = own + load_ref[z, c] * v
                    curve = curve + v * acc
                else:
                    image = au[0, z, c]
                    moved = u[0, z + 1, c] - alpha * v
                    own = own + (load_ref[z, c] - alpha * image) * moved
                    curve = curve + moved * (image - alpha * acc)
            return own, curve

        zero = jnp.zeros((nx, ny), jnp.float32)
        own, curve = lax.fori_loop(0, depth, plane, (zero, zero))
        for kind in (PLANE, PUSH, LOW, HIGH):
            arrive(it, kind)

        def change(z, c, rows, amount):
            v = u[it, z + 1, c, rows]
            if it == 0:
                return -(v * amount)
            step = alpha[rows]
            return (u[0, z + 1, c, rows] - step * v) * (step * amount)

        upper = sym_apply(cc, depth, [plane_recv[it, c] for c in range(4)])
        for c in range(4):
            au[it, depth - 1, c] = au[it, depth - 1, c] - upper[c]
            curve = curve + change(depth - 1, c, slice(0, nx), upper[c])
            lower = push_recv[it, c]
            au[it, 0, c] = au[it, 0, c] - lower
            curve = curve + change(0, c, slice(0, nx), lower)

        def edges(z, sums):
            for c in range(4):
                low = halo_recv[it, 0, z, c:c + 1]
                high = halo_recv[it, 1, z, c:c + 1]
                au[it, z, c, 0:1] = au[it, z, c, 0:1] - low
                au[it, z, c, nx - 1:nx] = au[it, z, c, nx - 1:nx] - high
                sums = sums + change(z, c, slice(0, 1), low)
                sums = sums + change(z, c, slice(nx - 1, nx), high)
            return sums

        crossing = lax.fori_loop(0, depth, edges, jnp.zeros((1, ny), jnp.float32))

        def narrow(row):
            folded = row[:, 0:128]
            for t in range(128, ny, 128):
                folded = folded + row[:, t:t + 128]
            return folded

        own = narrow(jnp.sum(own, axis=0, keepdims=True))
        curve = narrow(jnp.sum(curve, axis=0, keepdims=True) + crossing)
        row = lax.broadcasted_iota(jnp.int32, (8, 128), 0)
        tile = jnp.where(row < 4, jnp.broadcast_to(own, (8, 128)), jnp.broadcast_to(curve, (8, 128)))
        gbuf[it, me] = tile
        for k in range(1, n):
            gather(gbuf, gs_sem, gr_sem, "gz", me, it, k).start()
        deliver_image(it).start()

    def reduce_across(it):
        for k in range(1, n):
            gather(gbuf, gs_sem, gr_sem, "gz", me, it, k).wait_recv()
        tile = gbuf[it, 0]
        for k in range(1, n):
            tile = tile + gbuf[it, k]
        xbuf[it, side] = tile
        for k in range(1, m):
            gather(xbuf, xs_sem, xr_sem, "xy", side, it, k).start()

    def reduced(it):
        for k in range(1, m):
            gather(xbuf, xs_sem, xr_sem, "xy", side, it, k).wait_recv()
        tile = xbuf[it, 0]
        for k in range(1, m):
            tile = tile + xbuf[it, k]
        return (jnp.full((nx, ny), jnp.sum(tile[0:1]), jnp.float32),
                jnp.full((nx, ny), jnp.sum(tile[4:5]), jnp.float32))

    def gather(buf, ss, rs, axis, mine, it, k):
        return pltpu.make_async_remote_copy(
            src_ref=buf.at[it, mine], dst_ref=buf.at[it, mine], send_sem=ss.at[it, k],
            recv_sem=rs.at[it, k], device_id=neighbour(axis, k), device_id_type=MESH,
        )

    precondition(load_ref, 0)
    operate(0, None)
    precondition(au.at[0], 1)
    gamma, curve = reduced(0)
    alpha = gamma / curve
    operate(1, alpha)
    reduce_across(1)
    fresh, curve = reduced(1)
    beta = fresh / gamma
    second = fresh / (curve - beta * fresh / alpha)
    outer = alpha + second * (1.0 + beta)
    inner = second * alpha
    row = lax.broadcasted_iota(jnp.int32, (8, 128), 0)
    scalar_ref[...] = jnp.where(row < 4, outer[0:8, 0:128], inner[0:8, 0:128])
    for it in range(2):
        deliver(it).wait()
        deliver_image(it).wait()
    for it in range(2):
        for kind in range(6):
            @pl.when(senders[kind])
            def _(it=it, kind=kind):
                copy(it, kind).wait_send()
        for buf, ss, rs, axis, count, mine in (
            (gbuf, gs_sem, gr_sem, "gz", n, me), (xbuf, xs_sem, xr_sem, "xy", m, side)
        ):
            for k in range(1, count):
                gather(buf, ss, rs, axis, mine, it, k).wait_send()


def solution(mesh):
    n, m = mesh.shape["gz"], mesh.shape["xy"]

    def per_device(load, material, layers, stiffness, coupling, pivots, factor):
        depth, _, nx, ny = load.shape
        f32 = jnp.float32
        vmem = pl.BlockSpec(memory_space=pltpu.VMEM)
        smem = pl.BlockSpec(memory_space=pltpu.SMEM)
        dma = pltpu.SemaphoreType.DMA
        edge = pltpu.VMEM((2, 4, nx, ny), f32)
        hbm = pl.BlockSpec(memory_space=pl.ANY)
        base, image, turn, bend, scalars = pl.pallas_call(
            functools.partial(kernel, n, m),
            out_shape=(jax.ShapeDtypeStruct(load.shape, f32),) * 4
            + (jax.ShapeDtypeStruct((8, 128), f32),),
            in_specs=[vmem] * 3 + [smem] * 4,
            out_specs=(hbm,) * 4 + (vmem,),
            scratch_shapes=[
                pltpu.VMEM((depth, 10, nx, ny), f32),
                pltpu.VMEM((depth + 1, 10, nx, ny), f32),
                pltpu.VMEM((depth, 10, nx, ny), f32),
                pltpu.VMEM((depth, 16, nx, ny), f32),
                pltpu.VMEM((16, nx, ny), f32),
                pltpu.VMEM((2, depth + 2, 4, nx, ny), f32),
                pltpu.VMEM((2, depth, 4, nx, ny), f32),
                edge, edge, edge, edge, edge, edge, edge,
                pltpu.VMEM((2, 2, depth, 4, ny), f32),
                pltpu.VMEM((2, 2, depth, 4, ny), f32),
                pltpu.VMEM((2, n, 8, 128), f32),
                pltpu.VMEM((2, m, 8, 128), f32),
                dma((2, 6)), dma((2, 6)),
                dma((2, n)), dma((2, n)), dma((2, m)), dma((2, m)), dma((4,)),
            ],
            compiler_params=pltpu.CompilerParams(
                collective_id=0, has_side_effects=True, vmem_limit_bytes=58 * 1024 * 1024
            ),
            name="line_cg",
        )(load, material, layers, *(
            jnp.transpose(table, (1, 2, 0)) for table in (stiffness, coupling, pivots, factor)
        ))
        outer, inner = scalars[0, 0], scalars[4, 0]
        return outer * base - inner * turn, load - outer * image + inner * bend

    split = P("gz", None, "xy", None)
    labels = P("gz", "xy", None)
    return jax.shard_map(
        per_device,
        mesh=mesh,
        in_specs=(split, labels, labels, P(), P(), P(), P()),
        out_specs=(split, split),
        check_vma=False,
    )
```

```python
import functools

import jax
import jax.numpy as jnp
from jax import lax
from jax.experimental import pallas as pl
from jax.experimental.pallas import tpu as pltpu
from jax.sharding import PartitionSpec as P

MESH = pl.DeviceIdType.MESH
PAIRS = [(i, j) for i in range(4) for j in range(i, 4)]
SYM = {}
for _k, (_i, _j) in enumerate(PAIRS):
    SYM[_i, _j] = _k
    SYM[_j, _i] = _k
UP, DOWN, PUSH, PLANE, LOW, HIGH = range(6)


def pick(values, bits):
    level = 0
    while len(values) > 1:
        merged = []
        for i in range(0, len(values) - 1, 2):
            merged.append(jnp.where(bits[level], values[i + 1], values[i]))
        if len(values) % 2:
            merged.append(values[-1])
        values = merged
        level += 1
    return values[0]


def bit_masks(labels, entries):
    count = max(1, (entries - 1).bit_length())
    return [(labels & (1 << b)) != 0 for b in range(count)]


def total(terms):
    return (terms[0] + terms[1]) + (terms[2] + terms[3])


def kernel(
    n, m,
    load_ref, mat_ref, lay_ref, stiff_ref, coup_ref, piv_ref, fact_ref,
    base_ref, image_ref, turn_ref, bend_ref, scalar_ref,
    kc, cc, sc, pc, tc, u, au,
    up_send, up_recv, dn_send, dn_recv, push_send, push_recv, plane_recv,
    halo_send, halo_recv, gbuf, xbuf,
    send_sem, recv_sem, gs_sem, gr_sem, xs_sem, xr_sem, out_sem,
):
    depth, _, nx, ny = load_ref.shape
    me = lax.axis_index("gz")
    side = lax.axis_index("xy")
    not_first, not_last = me > 0, me < n - 1
    has_left, has_right = side > 0, side < m - 1

    barrier = pltpu.get_barrier_semaphore()
    for k in range(1, n):
        pl.semaphore_signal(
            barrier, inc=1, device_id={"gz": lax.rem(me + k, n)}, device_id_type=MESH
        )
    for k in range(1, m):
        pl.semaphore_signal(
            barrier, inc=1, device_id={"xy": lax.rem(side + k, m)}, device_id_type=MESH
        )

    def neighbour(axis, step):
        if axis == "gz":
            return {"gz": lax.rem(me + step + n, n)}
        return {"xy": lax.rem(side + step + m, m)}

    def remote(src, dst, it, kind, axis, step):
        return pltpu.make_async_remote_copy(
            src_ref=src, dst_ref=dst, send_sem=send_sem.at[it, kind],
            recv_sem=recv_sem.at[it, kind], device_id=neighbour(axis, step),
            device_id_type=MESH,
        )

    def copy(it, kind):
        if kind == UP:
            return remote(up_send.at[it], up_recv.at[it], it, UP, "gz", 1)
        if kind == DOWN:
            return remote(dn_send.at[it], dn_recv.at[it], it, DOWN, "gz", -1)
        if kind == PUSH:
            return remote(push_send.at[it], push_recv.at[it], it, PUSH, "gz", 1)
        if kind == PLANE:
            return remote(u.at[it, 1], plane_recv.at[it], it, PLANE, "gz", -1)
        if kind == LOW:
            return remote(halo_send.at[it, 0], halo_recv.at[it, 1], it, LOW, "xy", -1)
        return remote(halo_send.at[it, 1], halo_recv.at[it, 0], it, HIGH, "xy", 1)

    senders = {UP: not_last, DOWN: not_first, PUSH: not_last, PLANE: not_first,
               LOW: has_left, HIGH: has_right}
    receivers = {UP: not_first, DOWN: not_last, PUSH: not_first, PLANE: not_last,
                 LOW: has_right, HIGH: has_left}

    def start(it, kind):
        @pl.when(senders[kind])
        def _():
            copy(it, kind).start()

    def arrive(it, kind):
        @pl.when(receivers[kind])
        def _():
            copy(it, kind).wait_recv()

    zero_plane = jnp.zeros((4, nx, ny), jnp.float32)

    @pl.when(me == 0)
    def _():
        for it in range(2):
            up_recv[it] = zero_plane
            push_recv[it] = zero_plane

    @pl.when(me == n - 1)
    def _():
        for it in range(2):
            dn_recv[it] = zero_plane
            plane_recv[it] = zero_plane

    @pl.when(side == 0)
    def _():
        for it in range(2):
            halo_recv[it, 0] = jnp.zeros((depth, 4, ny), jnp.float32)

    @pl.when(side == m - 1)
    def _():
        for it in range(2):
            halo_recv[it, 1] = jnp.zeros((depth, 4, ny), jnp.float32)

    for it in range(2):
        u[it, 0] = zero_plane
        u[it, depth + 1] = zero_plane
    for k in range(10):
        cc[0, k] = jnp.zeros((nx, ny), jnp.float32)

    def fill(table, label_ref, out, entries_of, offset):
        entries = table.shape[2]

        def plane(z, carry):
            for t in range(0, ny, 128):
                bits = bit_masks(label_ref[z, :, t:t + 128], entries)
                for k, (i, j) in enumerate(entries_of):
                    values = [
                        jnp.full((nx, 128), table[i, j, e], jnp.float32) for e in range(entries)
                    ]
                    out[z + offset, k, :, t:t + 128] = pick(values, bits)
            return carry

        lax.fori_loop(0, depth, plane, 0)

    def fill_rest():
        fill(piv_ref, mat_ref, sc, PAIRS, 0)
        fill(stiff_ref, mat_ref, kc, PAIRS, 0)
        fill(coup_ref, lay_ref, cc, PAIRS, 1)

    fill(fact_ref, lay_ref, pc, [(i, j) for i in range(4) for j in range(4)], 0)

    def sym_apply(ref, z, v):
        return [total([ref[z, SYM[i, j]] * v[j] for j in range(4)]) for i in range(4)]

    def lift(z, v):
        return [total([pc[z, 4 * i + j] * v[j] for j in range(4)]) for i in range(4)]

    def drop(z, v):
        return [total([pc[z, 4 * j + i] * v[j] for j in range(4)]) for i in range(4)]

    def zeros4():
        return tuple(jnp.zeros((nx, ny), jnp.float32) for _ in range(4))

    def climb(src, it, z, carried, keep):
        moved = lift(z, carried)
        carried = [src[z, c] + moved[c] for c in range(4)]
        if keep:
            scaled = sym_apply(sc, z, carried)
            for c in range(4):
                u[it, z + 1, c] = scaled[c]
        return tuple(carried)

    def build_transfer():
        for x in range(0, nx, 8):
            for t in range(0, ny, 128):
                def level(z, now):
                    p = [pc[z, k, x:x + 8, t:t + 128] for k in range(16)]
                    return tuple(
                        total([p[4 * i + k] * now[4 * k + j] for k in range(4)])
                        for i in range(4) for j in range(4)
                    )

                now = tuple(pc[0, k, x:x + 8, t:t + 128] for k in range(16))
                now = lax.fori_loop(1, depth, level, now)
                for k in range(16):
                    tc[k, x:x + 8, t:t + 128] = now[k]

    def precondition(src, it):
        out = lax.fori_loop(
            0, depth, lambda z, c: climb(src, it, z, c, False), zeros4()
        )
        for c in range(4):
            up_send[it, c] = out[c]
        if it == 0:
            pl.semaphore_wait(barrier, n - 1 + m - 1)

        @pl.when(me == 0)
        def _():
            copy(it, UP).start()

        if it == 0:
            build_transfer()

            @pl.when(me >= n // 2)
            def _():
                fill_rest()

        @pl.when(not_first)
        def _():
            copy(it, UP).wait_recv()

            @pl.when(not_last)
            def _():
                for i in range(4):
                    moved = total([tc[4 * i + j] * up_recv[it, j] for j in range(4)])
                    up_send[it, i] = up_send[it, i] + moved
                copy(it, UP).start()

        if it == 0:
            @pl.when(me < n // 2)
            def _():
                fill_rest()

        else:
            reduce_across(it - 1)

        inflow = tuple(up_recv[it, c] for c in range(4))
        lax.fori_loop(0, depth, lambda z, c: climb(src, it, z, c, True), inflow)

        def fall(k, carried):
            z = depth - 1 - k
            return tuple(drop(z, [u[it, z + 1, c] + carried[c] for c in range(4)]))

        out = lax.fori_loop(0, depth, fall, zeros4())
        for c in range(4):
            dn_send[it, c] = out[c]

        @pl.when(me == n - 1)
        def _():
            copy(it, DOWN).start()

        @pl.when(not_last)
        def _():
            copy(it, DOWN).wait_recv()

            @pl.when(not_first)
            def _():
                for i in range(4):
                    moved = total([tc[4 * j + i] * dn_recv[it, j] for j in range(4)])
                    dn_send[it, i] = dn_send[it, i] + moved
                copy(it, DOWN).start()

        def settle(k, carried):
            z = depth - 1 - k
            now = [u[it, z + 1, c] + carried[c] for c in range(4)]
            for c in range(4):
                u[it, z + 1, c] = now[c]
            halo_send[it, 0, z] = jnp.concatenate([v[0:1] for v in now], axis=0)
            halo_send[it, 1, z] = jnp.concatenate([v[nx - 1:nx] for v in now], axis=0)
            return tuple(drop(z, now))

        inflow = tuple(dn_recv[it, c] for c in range(4))
        pushed = sym_apply(cc, depth, [u[it, depth, c] + inflow[c] for c in range(4)])
        for c in range(4):
            push_send[it, c] = pushed[c]
        start(it, PUSH)
        lax.fori_loop(0, depth, settle, inflow)
        start(it, LOW)
        start(it, HIGH)
        start(it, PLANE)
        deliver(it).start()

    def deliver(it):
        target = (base_ref, turn_ref)[it]
        return pltpu.make_async_copy(u.at[it, pl.ds(1, depth)], target, out_sem.at[it])

    def deliver_image(it):
        target = (image_ref, bend_ref)[it]
        return pltpu.make_async_copy(au.at[it], target, out_sem.at[2 + it])

    def operate(it, alpha):
        rows = lax.broadcasted_iota(jnp.int32, (nx, ny), 0)
        lanes = lax.broadcasted_iota(jnp.int32, (nx, ny), 1)

        def plane(z, carry):
            own, curve = carry
            here = [u[it, z + 1, c] for c in range(4)]
            above = [u[it, z + 2, c] for c in range(4)]
            below = [u[it, z, c] for c in range(4)]
            for c in range(4):
                v = here[c]
                acc = total([kc[z, SYM[c, j]] * here[j] for j in range(4)])
                acc = acc - total([cc[z + 1, SYM[c, j]] * above[j] for j in range(4)])
                acc = acc - total([cc[z, SYM[c, j]] * below[j] for j in range(4)])
                acc = acc - jnp.where(rows == 0, 0.0, pltpu.roll(v, 1, 0))
                acc = acc - jnp.where(rows == nx - 1, 0.0, pltpu.roll(v, nx - 1, 0))
                acc = acc - jnp.where(lanes == 0, 0.0, pltpu.roll(v, 1, 1))
                acc = acc - jnp.where(lanes == ny - 1, 0.0, pltpu.roll(v, ny - 1, 1))
                au[it, z, c] = acc
                if it == 0:
                    own = own + load_ref[z, c] * v
                    curve = curve + v * acc
                else:
                    image = au[0, z, c]
                    moved = u[0, z + 1, c] - alpha * v
                    own = own + (load_ref[z, c] - alpha * image) * moved
                    curve = curve + moved * (image - alpha * acc)
            return own, curve

        zero = jnp.zeros((nx, ny), jnp.float32)
        own, curve = lax.fori_loop(0, depth, plane, (zero, zero))
        for kind in (PLANE, PUSH, LOW, HIGH):
            arrive(it, kind)

        def change(z, c, rows, amount):
            v = u[it, z + 1, c, rows]
            if it == 0:
                return -(v * amount)
            step = alpha[rows]
            return (u[0, z + 1, c, rows] - step * v) * (step * amount)

        upper = sym_apply(cc, depth, [plane_recv[it, c] for c in range(4)])
        for c in range(4):
            au[it, depth - 1, c] = au[it, depth - 1, c] - upper[c]
            curve = curve + change(depth - 1, c, slice(0, nx), upper[c])
            lower = push_recv[it, c]
            au[it, 0, c] = au[it, 0, c] - lower
            curve = curve + change(0, c, slice(0, nx), lower)

        def edges(z, sums):
            for c in range(4):
                low = halo_recv[it, 0, z, c:c + 1]
                high = halo_recv[it, 1, z, c:c + 1]
                au[it, z, c, 0:1] = au[it, z, c, 0:1] - low
                au[it, z, c, nx - 1:nx] = au[it, z, c, nx - 1:nx] - high
                sums = sums + change(z, c, slice(0, 1), low)
                sums = sums + change(z, c, slice(nx - 1, nx), high)
            return sums

        crossing = lax.fori_loop(0, depth, edges, jnp.zeros((1, ny), jnp.float32))

        def narrow(row):
            folded = row[:, 0:128]
            for t in range(128, ny, 128):
                folded = folded + row[:, t:t + 128]
            return folded

        own = narrow(jnp.sum(own, axis=0, keepdims=True))
        curve = narrow(jnp.sum(curve, axis=0, keepdims=True) + crossing)
        row = lax.broadcasted_iota(jnp.int32, (8, 128), 0)
        tile = jnp.where(row < 4, jnp.broadcast_to(own, (8, 128)), jnp.broadcast_to(curve, (8, 128)))
        gbuf[it, me] = tile
        for k in range(1, n):
            gather(gbuf, gs_sem, gr_sem, "gz", me, it, k).start()
        deliver_image(it).start()

    def reduce_across(it):
        for k in range(1, n):
            gather(gbuf, gs_sem, gr_sem, "gz", me, it, k).wait_recv()
        tile = gbuf[it, 0]
        for k in range(1, n):
            tile = tile + gbuf[it, k]
        xbuf[it, side] = tile
        for k in range(1, m):
            gather(xbuf, xs_sem, xr_sem, "xy", side, it, k).start()

    def reduced(it):
        for k in range(1, m):
            gather(xbuf, xs_sem, xr_sem, "xy", side, it, k).wait_recv()
        tile = xbuf[it, 0]
        for k in range(1, m):
            tile = tile + xbuf[it, k]
        return (jnp.full((nx, ny), jnp.sum(tile[0:1]), jnp.float32),
                jnp.full((nx, ny), jnp.sum(tile[4:5]), jnp.float32))

    def gather(buf, ss, rs, axis, mine, it, k):
        return pltpu.make_async_remote_copy(
            src_ref=buf.at[it, mine], dst_ref=buf.at[it, mine], send_sem=ss.at[it, k],
            recv_sem=rs.at[it, k], device_id=neighbour(axis, k), device_id_type=MESH,
        )

    precondition(load_ref, 0)
    operate(0, None)
    precondition(au.at[0], 1)
    gamma, curve = reduced(0)
    alpha = gamma / curve
    operate(1, alpha)
    reduce_across(1)
    fresh, curve = reduced(1)
    beta = fresh / gamma
    second = fresh / (curve - beta * fresh / alpha)
    outer = alpha + second * (1.0 + beta)
    inner = second * alpha
    row = lax.broadcasted_iota(jnp.int32, (8, 128), 0)
    scalar_ref[...] = jnp.where(row < 4, outer[0:8, 0:128], inner[0:8, 0:128])
    for it in range(2):
        deliver(it).wait()
        deliver_image(it).wait()
    for it in range(2):
        for kind in range(6):
            @pl.when(senders[kind])
            def _(it=it, kind=kind):
                copy(it, kind).wait_send()
        for buf, ss, rs, axis, count, mine in (
            (gbuf, gs_sem, gr_sem, "gz", n, me), (xbuf, xs_sem, xr_sem, "xy", m, side)
        ):
            for k in range(1, count):
                gather(buf, ss, rs, axis, mine, it, k).wait_send()


def combine(scalars, base, turn, load, image, bend, sol_ref, res_ref):
    outer, inner = scalars[0, 0], scalars[4, 0]
    sol_ref[...] = outer * base[...] - inner * turn[...]
    res_ref[...] = load[...] - outer * image[...] + inner * bend[...]


def solution(mesh):
    n, m = mesh.shape["gz"], mesh.shape["xy"]

    def per_device(load, material, layers, stiffness, coupling, pivots, factor):
        depth, _, nx, ny = load.shape
        f32 = jnp.float32
        vmem = pl.BlockSpec(memory_space=pltpu.VMEM)
        smem = pl.BlockSpec(memory_space=pltpu.SMEM)
        dma = pltpu.SemaphoreType.DMA
        edge = pltpu.VMEM((2, 4, nx, ny), f32)
        hbm = pl.BlockSpec(memory_space=pl.ANY)
        base, image, turn, bend, scalars = pl.pallas_call(
            functools.partial(kernel, n, m),
            out_shape=(jax.ShapeDtypeStruct(load.shape, f32),) * 4
            + (jax.ShapeDtypeStruct((8, 128), f32),),
            in_specs=[vmem] * 3 + [smem] * 4,
            out_specs=(hbm,) * 4 + (vmem,),
            scratch_shapes=[
                pltpu.VMEM((depth, 10, nx, ny), f32),
                pltpu.VMEM((depth + 1, 10, nx, ny), f32),
                pltpu.VMEM((depth, 10, nx, ny), f32),
                pltpu.VMEM((depth, 16, nx, ny), f32),
                pltpu.VMEM((16, nx, ny), f32),
                pltpu.VMEM((2, depth + 2, 4, nx, ny), f32),
                pltpu.VMEM((2, depth, 4, nx, ny), f32),
                edge, edge, edge, edge, edge, edge, edge,
                pltpu.VMEM((2, 2, depth, 4, ny), f32),
                pltpu.VMEM((2, 2, depth, 4, ny), f32),
                pltpu.VMEM((2, n, 8, 128), f32),
                pltpu.VMEM((2, m, 8, 128), f32),
                dma((2, 6)), dma((2, 6)),
                dma((2, n)), dma((2, n)), dma((2, m)), dma((2, m)), dma((4,)),
            ],
            compiler_params=pltpu.CompilerParams(
                collective_id=0, has_side_effects=True, vmem_limit_bytes=58 * 1024 * 1024
            ),
            name="line_cg",
        )(load, material, layers, *(
            jnp.transpose(table, (1, 2, 0)) for table in (stiffness, coupling, pivots, factor)
        ))
        planes = 4 if depth % 4 == 0 else 1
        block = pl.BlockSpec((planes, 4, nx, ny), lambda z: (z, 0, 0, 0))
        return pl.pallas_call(
            combine,
            grid=(depth // planes,),
            out_shape=(jax.ShapeDtypeStruct(load.shape, f32),) * 2,
            in_specs=[smem] + [block] * 5,
            out_specs=(block, block),
            name="combine",
        )(scalars, base, turn, load, image, bend)

    split = P("gz", None, "xy", None)
    labels = P("gz", "xy", None)
    return jax.shard_map(
        per_device,
        mesh=mesh,
        in_specs=(split, labels, labels, P(), P(), P(), P()),
        out_specs=(split, split),
        check_vma=False,
    )
```
